8 devices in a mesh: data: 2 (over z, y), fsdp: 2 (over x), model: 2 (over core).
Axes of the slice: x: 2, y: 2, z: 1, core: 2. Of those that a mesh axis runs over, the one named last changes fastest.
Arguments:
- x_in: bfloat16 [128, 128, 2048], P(('data', 'fsdp'), 'model')
- grad_out: bfloat16 [128, 128, 2048], P(('data', 'fsdp'), 'model')
- gain_attn: float32 [2048], replicated
- gain_mlp: float32 [2048], replicated
- w_qkv: bfloat16 [2048, 3072], P(('data', 'fsdp'), 'model')
- w_out: bfloat16 [2048, 2048], P('model', ('data', 'fsdp'))
- w_gate: bfloat16 [2048, 8192], P(('data', 'fsdp'), 'model')
- w_up: bfloat16 [2048, 8192], P(('data', 'fsdp'), 'model')
- w_down: bfloat16 [8192, 2048], P('model', ('data', 'fsdp'))
- rope_cos: float32 [128, 32], replicated
- rope_sin: float32 [128, 32], replicated
Outputs:
- output 1: bfloat16 [128, 128, 2048], P(('data', 'fsdp'), 'model')
- output 2: bfloat16 [128, 128, 2048], P(('data', 'fsdp'), 'model')
- output 3: float32 [2048, 3072], P(('data', 'fsdp'), 'model')
- output 4: float32 [2048, 2048], P('model', ('data', 'fsdp'))
- output 5: float32 [2048, 8192], P(('data', 'fsdp'), 'model')
- output 6: float32 [2048, 8192], P(('data', 'fsdp'), 'model')
- output 7: float32 [8192, 2048], P('model', ('data', 'fsdp'))
All inputs are finite; a program needn't handle non-finite values.
Results may differ from the reference program's by a relative error of at most 0.0170236.
Values are sent between devices in bfloat16 or wider.
A program may use at most 1 GiB of HBM per device.

```python
import jax
import jax.numpy as jnp
from jax import lax

D_MODEL = 2048
FFN_DIM = 8192
Q_HEADS = 32
KV_HEADS = 8
HEAD_DIM = 64
GLOBAL_BATCH = 128
SEQ_LEN = 128


def setup_inputs(seed: int = 0) -> dict:
    key_list = jax.random.split(jax.random.key(seed), 11)
    qkv_width = (Q_HEADS + 2 * KV_HEADS) * HEAD_DIM
    attn_width = Q_HEADS * HEAD_DIM
    half_dim = HEAD_DIM // 2
    act_shape = (GLOBAL_BATCH, SEQ_LEN, D_MODEL)
    x_in = jax.random.normal(key_list[0], act_shape, jnp.float32).astype(jnp.bfloat16)
    grad_out = jax.random.normal(key_list[1], act_shape, jnp.float32).astype(jnp.bfloat16)
    gain_attn = jax.random.uniform(key_list[2], (D_MODEL,), jnp.float32, 0.5, 1.5)
    gain_mlp = jax.random.uniform(key_list[3], (D_MODEL,), jnp.float32, 0.5, 1.5)
    w_qkv = (jax.random.normal(key_list[4], (D_MODEL, qkv_width), jnp.float32) * D_MODEL ** -0.5).astype(jnp.bfloat16)
    w_out = (jax.random.normal(key_list[5], (attn_width, D_MODEL), jnp.float32) * attn_width ** -0.5).astype(jnp.bfloat16)
    w_gate = (jax.random.normal(key_list[6], (D_MODEL, FFN_DIM), jnp.float32) * D_MODEL ** -0.5).astype(jnp.bfloat16)
    w_up = (jax.random.normal(key_list[7], (D_MODEL, FFN_DIM), jnp.float32) * D_MODEL ** -0.5).astype(jnp.bfloat16)
    w_down = (jax.random.normal(key_list[8], (FFN_DIM, D_MODEL), jnp.float32) * FFN_DIM ** -0.5).astype(jnp.bfloat16)
    base_freq = 10000.0 ** (-jnp.arange(half_dim, dtype=jnp.float32) / half_dim)
    inv_freq = base_freq * jax.random.uniform(key_list[9], (half_dim,), jnp.float32, 0.5, 2.0)
    start_pos = jax.random.randint(key_list[10], (), 0, 4096)
    positions = (jnp.arange(SEQ_LEN) + start_pos).astype(jnp.float32)
    angles = positions[:, None] * inv_freq[None, :]
    return {'x_in': x_in, 'grad_out': grad_out, 'gain_attn': gain_attn, 'gain_mlp': gain_mlp,
            'w_qkv': w_qkv, 'w_out': w_out, 'w_gate': w_gate, 'w_up': w_up, 'w_down': w_down,
            'rope_cos': jnp.cos(angles), 'rope_sin': jnp.sin(angles)}


def rms_norm(x_f32, gain_vec):
    mean_sq = jnp.mean(x_f32 * x_f32, axis=-1, keepdims=True)
    return (x_f32 * lax.rsqrt(mean_sq + 1e-5) * gain_vec).astype(jnp.bfloat16)


def rotate_qk(qkv_proj, rope_cos, rope_sin):
    half_dim = HEAD_DIM // 2
    cos_b = rope_cos[None, :, None, None, :]
    sin_b = rope_sin[None, :, None, None, :]
    qk_part = qkv_proj[:, :, :, :-1]
    lo_half = qk_part[..., :half_dim]
    hi_half = qk_part[..., half_dim:]
    rotated = jnp.concatenate([lo_half * cos_b - hi_half * sin_b, hi_half * cos_b + lo_half * sin_b], axis=-1).astype(jnp.bfloat16)
    return rotated[:, :, :, :-1], rotated[:, :, :, -1], qkv_proj[:, :, :, -1].astype(jnp.bfloat16)


def attend_group(group_in):
    q_grp, k_grp, v_grp = group_in
    scores = jnp.einsum('sgd,td->gst', q_grp.astype(jnp.float32), k_grp.astype(jnp.float32)) * (HEAD_DIM ** -0.5)
    causal = jnp.arange(SEQ_LEN)[:, None] >= jnp.arange(SEQ_LEN)[None, :]
    scores = jnp.where(causal, scores, -1e30)
    attn_probs = jax.nn.softmax(scores, axis=-1).astype(jnp.bfloat16)
    attn_mix = jnp.einsum('gst,td->sgd', attn_probs.astype(jnp.float32), v_grp.astype(jnp.float32))
    return attn_mix.astype(jnp.bfloat16)


def decoder_layer(x_in, gain_attn, gain_mlp, w_qkv, w_out, w_gate, w_up, w_down, rope_cos, rope_sin):
    group_size = Q_HEADS // KV_HEADS
    row_count = GLOBAL_BATCH * SEQ_LEN
    x_f32 = x_in.astype(jnp.float32)
    h_attn = rms_norm(x_f32, gain_attn).reshape(row_count, D_MODEL).astype(jnp.float32)
    qkv_proj = jnp.dot(h_attn, w_qkv, preferred_element_type=jnp.float32)
    qkv_proj = qkv_proj.reshape(GLOBAL_BATCH, SEQ_LEN, KV_HEADS, group_size + 2, HEAD_DIM)
    q_rot, k_rot, v_val = rotate_qk(qkv_proj, rope_cos, rope_sin)
    q_grp = q_rot.transpose(0, 2, 1, 3, 4).reshape(GLOBAL_BATCH * KV_HEADS, SEQ_LEN, group_size, HEAD_DIM)
    k_grp = k_rot.transpose(0, 2, 1, 3).reshape(GLOBAL_BATCH * KV_HEADS, SEQ_LEN, HEAD_DIM)
    v_grp = v_val.transpose(0, 2, 1, 3).reshape(GLOBAL_BATCH * KV_HEADS, SEQ_LEN, HEAD_DIM)
    attn_mix = lax.map(jax.checkpoint(attend_group), (q_grp, k_grp, v_grp))
    attn_mix = attn_mix.reshape(GLOBAL_BATCH, KV_HEADS, SEQ_LEN, group_size, HEAD_DIM).transpose(0, 2, 1, 3, 4)
    attn_in = attn_mix.reshape(row_count, Q_HEADS * HEAD_DIM).astype(jnp.float32)
    attn_proj = jnp.dot(attn_in, w_out, preferred_element_type=jnp.float32).astype(jnp.bfloat16)
    y_mid = (x_f32 + attn_proj.astype(jnp.float32).reshape(x_in.shape)).astype(jnp.bfloat16)
    mid_f32 = y_mid.astype(jnp.float32)
    h_mlp = rms_norm(mid_f32, gain_mlp).reshape(row_count, D_MODEL).astype(jnp.float32)
    gate_val = jnp.dot(h_mlp, w_gate, preferred_element_type=jnp.float32)
    up_val = jnp.dot(h_mlp, w_up, preferred_element_type=jnp.float32)
    act_val = (jax.nn.silu(gate_val) * up_val).astype(jnp.bfloat16)
    mlp_proj = jnp.dot(act_val.astype(jnp.float32), w_down, preferred_element_type=jnp.float32).astype(jnp.bfloat16)
    return (mid_f32 + mlp_proj.astype(jnp.float32).reshape(x_in.shape)).astype(jnp.bfloat16)


def reference(x_in, grad_out, gain_attn, gain_mlp, w_qkv, w_out, w_gate, w_up, w_down, rope_cos, rope_sin):
    def layer_fn(x_val, w_vals):
        return decoder_layer(x_val, gain_attn, gain_mlp, w_vals[0], w_vals[1], w_vals[2], w_vals[3], w_vals[4], rope_cos, rope_sin)
    weight_list = [w_qkv.astype(jnp.float32), w_out.astype(jnp.float32), w_gate.astype(jnp.float32),
                   w_up.astype(jnp.float32), w_down.astype(jnp.float32)]
    y_out, pull_back = jax.vjp(layer_fn, x_in, weight_list)
    dx_in, weight_grads = pull_back(grad_out)
    return (y_out, dx_in, weight_grads[0], weight_grads[1], weight_grads[2], weight_grads[3], weight_grads[4])
```

```python
import functools
import jax
import jax.numpy as jnp
from jax import lax
from jax.experimental import pallas as pl
from jax.experimental.pallas import tpu as pltpu
from jax.sharding import PartitionSpec as P

FSDP_AXES = ('data', 'fsdp')
SWAP = ((0, 1), (1, 0))
F32 = jnp.float32
BF16 = jnp.bfloat16
NN = (((1,), (0,)), ((), ()))
NT = (((1,), (1,)), ((), ()))
TN = (((0,), (0,)), ((), ()))
ANY = pl.BlockSpec(memory_space=pl.ANY)
EPS = 1e-5
HEAD = 64


def dot(a, b, dims=NN):
    return lax.dot_general(a, b, dims, preferred_element_type=F32)


def params(mib=60):
    return pltpu.CompilerParams(vmem_limit_bytes=mib * 1024 * 1024)


def cost(flops, nbytes, trans=0):
    return pl.CostEstimate(flops=int(flops), bytes_accessed=int(nbytes), transcendentals=int(trans))


def scalar_call(body, grid, in_specs, out_specs, out_shape, scratch=(), alias=None, ce=None):
    return pl.pallas_call(
        body, out_shape=out_shape,
        grid_spec=pltpu.PrefetchScalarGridSpec(num_scalar_prefetch=1, grid=grid, in_specs=in_specs, out_specs=out_specs,
                                               scratch_shapes=list(scratch)),
        input_output_aliases=alias or {}, compiler_params=params(), cost_estimate=ce)


class Weight:
    def __init__(self, shape, axis, pieces):
        self.shape, self.axis, self.pieces = shape, axis, pieces

    def arrays(self):
        return [p[0] for p in self.pieces]

    def copies(self, ids, refs, dst, sem, base):
        blk = self.shape[self.axis] // 4
        out = []
        for i, (ref, (arr, j, off)) in enumerate(zip(refs, self.pieces)):
            n = arr.shape[1 - self.axis]
            at = [pl.ds(off, n), pl.ds(off, n)]
            at[self.axis] = pl.ds(pl.multiple_of(ids[j] * blk, blk), blk)
            out.append(pltpu.make_async_copy(ref, dst.at[at[0], at[1]], sem.at[base + i]))
        return out


def load_all(ids, weights, refs, dsts, sem):
    copies, n = [], 0
    for w, dst in zip(weights, dsts):
        copies += w.copies(ids, refs[n:n + len(w.pieces)], dst, sem, n)
        n += len(w.pieces)
    for c in copies:
        c.start()
    for c in copies:
        c.wait()


def weight_scratch(weights):
    return [pltpu.VMEM(w.shape, BF16) for w in weights] + [pltpu.SemaphoreType.DMA((sum(len(w.pieces) for w in weights),))]


def rms_f(v, gain):
    return (v * lax.rsqrt(jnp.mean(v * v, axis=-1, keepdims=True) + EPS) * gain).astype(BF16)


def rms_b(v, gain, dh):
    r = lax.rsqrt(jnp.mean(v * v, axis=-1, keepdims=True) + EPS)
    gd = gain * dh
    return r * gd - v * (r * r * r * jnp.mean(v * gd, axis=-1, keepdims=True))


def rms_kernel(x_ref, gain_ref, h_ref):
    h_ref[...] = rms_f(x_ref[...].astype(F32), gain_ref[...])


def rms_call(x, gain, tile=256):
    t, d = x.shape
    row = pl.BlockSpec((tile, d), lambda i: (i, 0))
    return pl.pallas_call(rms_kernel, grid=(t // tile,), in_specs=[row, pl.BlockSpec((1, d), lambda i: (0, 0))],
                          out_specs=row, out_shape=jax.ShapeDtypeStruct((t, d), BF16), compiler_params=params(),
                          cost_estimate=cost(t * d * 8, 4 * t * d))(x, gain)


def rope(x, c, s, sign):
    lane = lax.broadcasted_iota(jnp.int32, x.shape, x.ndim - 1)
    partner = jnp.where(lane % HEAD < HEAD // 2, pltpu.roll(x, 96, x.ndim - 1), pltpu.roll(x, 32, x.ndim - 1))
    return x * c + (partner * s if sign > 0 else -(partner * s))


def qkv_kernel(w, seq_loc, ids, h_ref, c_ref, s_ref, *refs):
    n = len(w.pieces)
    out, wv, sem = refs[n:]

    @pl.when(pl.program_id(0) == 0)
    def _():
        load_all(ids, [w], refs[:n], [wv], sem)

    h = h_ref[...]
    nb = h.shape[0] // seq_loc
    for g in range(w.shape[1] // 768):
        acc = dot(h, wv[:, g * 768:(g + 1) * 768])
        for q in range(6):
            k = q % 3
            part = acc[:, q * 128:(q + 1) * 128].reshape(nb, seq_loc, 128)
            cs = c_ref[0, :, k * 128:(k + 1) * 128][None]
            sn = s_ref[0, :, k * 128:(k + 1) * 128][None]
            lo = g * 768 + q * 128
            out[:, lo:lo + 128] = rope(part, cs, sn, 1).astype(BF16).reshape(nb * seq_loc, 128)


def qkv_call(ids, h, w, cos_t, sin_t, tile=512):
    t, d = h.shape
    width = w.shape[1]
    seq_loc = cos_t.shape[1]
    nt = t // tile
    tab = pl.BlockSpec((1, seq_loc, 384), lambda i, s: (i * 2 // nt, 0, 0))
    return scalar_call(functools.partial(qkv_kernel, w, seq_loc), (nt,),
                       [pl.BlockSpec((tile, d), lambda i, s: (i, 0)), tab, tab] + [ANY] * len(w.pieces),
                       pl.BlockSpec((tile, width), lambda i, s: (i, 0)), jax.ShapeDtypeStruct((t, width), BF16),
                       weight_scratch([w]), ce=cost(2 * t * d * width, 2 * (t * d + d * width + t * width)))(
        ids, h, cos_t, sin_t, *w.arrays())


def spread(kv):
    f = kv.astype(F32)
    lane = lax.broadcasted_iota(jnp.int32, f.shape, 1)
    k0 = jnp.where(lane < HEAD, f, 0.0)
    v1 = jnp.where(lane < HEAD, 0.0, f)
    kz = jnp.concatenate([k0, pltpu.roll(k0, HEAD, 1)], axis=0).astype(BF16)
    vz = jnp.concatenate([pltpu.roll(v1, HEAD, 1), v1], axis=0).astype(BF16)
    return kz, vz


def probs(q, kz, seq):
    s = dot(kz, q, NT) * (HEAD ** -0.5)
    t = lax.broadcasted_iota(jnp.int32, (seq, 2 * seq), 0)
    pos = lax.broadcasted_iota(jnp.int32, (seq, 2 * seq), 1) % seq
    out = []
    for h in range(2):
        sh = jnp.where(pos >= t, s[h * seq:(h + 1) * seq], -1e30)
        e = jnp.exp(sh - jnp.max(sh, axis=0, keepdims=True))
        out.append(e * (1.0 / jnp.sum(e, axis=0, keepdims=True)))
    return out


def pair_rows(ref, b, seq, first):
    lo = ref[:, b, :, first:first + 128].reshape(seq, 128)
    hi = ref[:, b, :, first + 128:first + 256].reshape(seq, 128)
    return jnp.concatenate([lo, hi], axis=0)


def attn_kernel(nb, seq, qkv_ref, o_ref):
    half = seq // 2
    for b in range(nb):
        q = pair_rows(qkv_ref, b, seq, 0)
        kz, vz = spread(qkv_ref[:, b, :, 256:384].reshape(seq, 128))
        p = jnp.concatenate(probs(q, kz, seq), axis=0).astype(BF16)
        o = dot(p, vz, TN).astype(BF16)
        o_ref[:, b, :, 0:128] = o[:seq].reshape(2, half, 128)
        o_ref[:, b, :, 128:256] = o[seq:].reshape(2, half, 128)


def attn_call(qkv, nb=16):
    two, batch, half, width = qkv.shape
    groups = width // 384
    seq = two * half
    spec = lambda n: pl.BlockSpec((2, nb, half, n), lambda i, j: (0, i, 0, j))
    return pl.pallas_call(functools.partial(attn_kernel, nb, seq), grid=(batch // nb, groups), in_specs=[spec(384)],
                          out_specs=spec(256), out_shape=jax.ShapeDtypeStruct((2, batch, half, groups * 256), BF16),
                          compiler_params=params(), cost_estimate=cost(8e9, 20e6, 4e6))(qkv)


def attn_bwd_kernel(nb, seq, qkv_ref, do_ref, c_ref, s_ref, out_ref):
    half = seq // 2
    cos_t = [c_ref[:, :, k * 128:(k + 1) * 128].reshape(seq, 128) for k in range(3)]
    sin_t = [s_ref[:, :, k * 128:(k + 1) * 128].reshape(seq, 128) for k in range(3)]
    for b in range(nb):
        q = pair_rows(qkv_ref, b, seq, 0)
        do = pair_rows(do_ref, b, seq, 0)
        kz, vz = spread(qkv_ref[:, b, :, 256:384].reshape(seq, 128))
        ps = probs(q, kz, seq)
        dp = dot(vz, do, NT)
        ds = []
        for h in range(2):
            d = dp[h * seq:(h + 1) * seq].astype(BF16).astype(F32)
            ds.append(ps[h] * (d - jnp.sum(ps[h] * d, axis=0, keepdims=True)) * (HEAD ** -0.5))
        ds = jnp.concatenate(ds, axis=0).astype(BF16)
        p = jnp.concatenate(ps, axis=0).astype(BF16)
        dq = dot(ds, kz, TN).astype(BF16).astype(F32)
        rk = dot(ds, q)
        rv = dot(p, do)
        lane = lax.broadcasted_iota(jnp.int32, (seq, 128), 1)
        dkv = jnp.where(lane < HEAD, rk[:seq] + pltpu.roll(rk[seq:], HEAD, 1), pltpu.roll(rv[:seq], HEAD, 1) + rv[seq:])
        dkv = dkv.astype(BF16).astype(F32)
        for k, part in enumerate((dq[:seq], dq[seq:], dkv)):
            out_ref[:, b, :, k * 128:(k + 1) * 128] = rope(part, cos_t[k], sin_t[k], -1).astype(BF16).reshape(2, half, 128)


def attn_bwd_call(qkv, d_o, cos_t, sin_t, nb=8):
    two, batch, half, width = qkv.shape
    groups = width // 384
    seq = two * half
    spec = lambda n: pl.BlockSpec((2, nb, half, n), lambda i, j: (0, i, 0, j))
    tab = pl.BlockSpec((2, half, 384), lambda i, j: (0, 0, 0))
    return pl.pallas_call(functools.partial(attn_bwd_kernel, nb, seq), grid=(batch // nb, groups),
                          in_specs=[spec(384), spec(256), tab, tab], out_specs=spec(384),
                          out_shape=jax.ShapeDtypeStruct(qkv.shape, BF16), compiler_params=params(),
                          cost_estimate=cost(20e9, 40e6, 8e6))(qkv, d_o, cos_t, sin_t)


def mlp_kernel(ws, nc, ids, h_ref, g_ref, *refs):
    n = sum(len(w.pieces) for w in ws)
    act_ref, dgu_ref, wgu, wd, sem = refs[n:]

    @pl.when(pl.program_id(0) == 0)
    def _():
        load_all(ids, ws, refs[:n], [wgu, wd], sem)

    width = wd.shape[0]
    step = width // nc
    h = h_ref[...]
    g = g_ref[...]
    for c in range(nc):
        cols, ucols = pl.ds(c * step, step), pl.ds(width + c * step, step)
        gate = dot(h, wgu[:, cols])
        up = dot(h, wgu[:, ucols])
        d_act = dot(g, wd[cols, :], NT).astype(BF16).astype(F32)
        sig = jax.nn.sigmoid(gate)
        gate_act = gate * sig
        act_ref[:, cols] = (gate_act * up).astype(BF16)
        dgu_ref[:, ucols] = (d_act * gate_act).astype(BF16)
        dgu_ref[:, cols] = (d_act * up * sig * (1.0 + gate * (1.0 - sig))).astype(BF16)


def mlp_call(ids, h, g, wgu, wd, tile=512, nc=8):
    t, d = h.shape
    f = wd.shape[0]
    row = lambda n: pl.BlockSpec((tile, n), lambda i, s: (i, 0))
    ws = [wgu, wd]
    arrs = wgu.arrays() + wd.arrays()
    return scalar_call(functools.partial(mlp_kernel, ws, nc), (t // tile,), [row(d), row(d)] + [ANY] * len(arrs),
                       [row(f), row(2 * f)], [jax.ShapeDtypeStruct((t, f), BF16), jax.ShapeDtypeStruct((t, 2 * f), BF16)],
                       weight_scratch(ws), ce=cost(6 * t * d * f, 4 * t * d + 6 * d * f + 6 * t * f, t * f))(ids, h, g, *arrs)


def proj_kernel(ws, dims, n_extra, epi, ids, *refs):
    k = len(ws)
    n = sum(len(w.pieces) for w in ws)
    lhs, extra, pieces = refs[:k], refs[k:k + n_extra], refs[k + n_extra:k + n_extra + n]
    outs, dsts, sem = refs[k + n_extra + n:-k - 1], refs[-k - 1:-1], refs[-1]
    first = pl.program_id(0) == 0

    def body(waits):
        acc = None
        for i in range(k):
            for c in waits[i]:
                c.wait()
            for lo in range(0, lhs[i].shape[1], 2048):
                part = pl.ds(lo, min(2048, lhs[i].shape[1]))
                d = dot(lhs[i][:, part], dsts[i][part, :] if dims is NN else dsts[i][:, part], dims)
                acc = d if acc is None else acc + d
        epi(acc, extra, outs)

    @pl.when(first)
    def _():
        groups, m = [], 0
        for w, dst in zip(ws, dsts):
            groups.append(w.copies(ids, pieces[m:m + len(w.pieces)], dst, sem, m))
            m += len(w.pieces)
        for c in sum(groups, []):
            c.start()
        body(groups)

    @pl.when(jnp.logical_not(first))
    def _():
        body([[]] * k)


def proj_call(ids, lhs, ws, dims, rows, which, epi, extra, outs, tile=256):
    t = rows
    kdim = lhs[0].shape[1]
    nout = ws[0].shape[1] if dims is NN else ws[0].shape[0]
    nt = t // tile
    if which is None:
        lrow = pl.BlockSpec((tile, kdim), lambda i, s: (i, 0))
    else:
        lrow = pl.BlockSpec((tile, kdim), lambda i, s: (s[which] * nt + i, 0))
    row = pl.BlockSpec((tile, nout), lambda i, s: (i, 0))
    espec = [row if e.shape[0] == t else pl.BlockSpec((1, nout), lambda i, s: (0, 0)) for e in extra]
    arrs = sum([w.arrays() for w in ws], [])
    return scalar_call(functools.partial(proj_kernel, ws, dims, len(extra), epi), (nt,),
                       [lrow] * len(lhs) + espec + [ANY] * len(arrs), [row] * outs,
                       [jax.ShapeDtypeStruct((t, nout), BF16)] * outs, weight_scratch(ws),
                       ce=cost(2 * t * kdim * nout * len(ws), 2 * len(ws) * (t * kdim + kdim * nout) + 2 * t * nout * (outs + len(extra))))(
        ids, *lhs, *extra, *arrs)


def epi_round(acc, extra, outs):
    outs[0][...] = acc.astype(BF16)


def epi_mid(acc, extra, outs):
    recv, x, gain = extra
    s = (acc + recv[...].astype(F32)).astype(BF16).astype(F32)
    mid = (x[...].astype(F32) + s).astype(BF16)
    outs[0][...] = mid
    outs[1][...] = rms_f(mid.astype(F32), gain[...])


def epi_add(acc, extra, outs):
    recv, mid = extra
    s = (acc + recv[...].astype(F32)).astype(BF16).astype(F32)
    outs[0][...] = (mid[...].astype(F32) + s).astype(BF16)


def epi_rms_b(acc, extra, outs):
    recv, v, res, gain = extra
    dh = (acc + recv[...].astype(F32)).astype(BF16).astype(F32)
    outs[0][...] = (res[...].astype(F32) + rms_b(v[...].astype(F32), gain[...], dh)).astype(BF16)


def tn_kernel(adds, ids, a_ref, b_ref, *refs):
    out = refs[-1]
    acc = dot(a_ref[...], b_ref[...], TN)
    for i in range(adds):
        acc += refs[i][...]
    out[...] = acc


def tn_call(ids, a, b, side, blocks, adds=(), into=None, out_shape=None, place=0):
    t = a.shape[0]
    dblk = 512
    nb = len(blocks)
    other = (b if side == 0 else a).shape[1]
    ot = (1024 if other % 1024 == 0 else 768) if side == 0 else 512
    no = other // ot

    def dsel(i, s):
        v = s[blocks[0]]
        for k in range(1, nb):
            v = jnp.where(i == k, s[blocks[k]], v)
        return v

    if side == 0:
        a_spec = pl.BlockSpec((t, dblk), lambda j, i, s: (0, dsel(i, s)))
        b_spec = pl.BlockSpec((t, ot), lambda j, i, s: (0, j))
        blk, add_map = (dblk, ot), lambda j, i, s: (i, j)
        shape, off = (nb * dblk, other), place // ot
        out_map = lambda j, i, s: (i, j + off)
    else:
        a_spec = pl.BlockSpec((t, ot), lambda j, i, s: (0, j))
        b_spec = pl.BlockSpec((t, dblk), lambda j, i, s: (0, dsel(i, s)))
        blk, add_map = (ot, dblk), lambda j, i, s: (j, i)
        shape, off = (other, nb * dblk), place // ot
        out_map = lambda j, i, s: (j + off, i)
    shape = out_shape or shape
    extra_in, extra_spec, alias = [], [], None
    if into is not None:
        extra_in, extra_spec, alias = [into], [ANY], {3 + len(adds): 0}
    return scalar_call(functools.partial(tn_kernel, len(adds)), (no, nb),
                       [a_spec, b_spec] + [pl.BlockSpec(blk, add_map)] * len(adds) + extra_spec, pl.BlockSpec(blk, out_map),
                       jax.ShapeDtypeStruct(shape, F32), alias=alias,
                       ce=cost(2 * t * nb * dblk * other, 2 * t * (nb * dblk + other) + 4 * nb * dblk * other * (1 + len(adds))))(
        ids, a, b, *adds, *extra_in)


def tn2_kernel(adds, half, ids, a_ref, b_ref, *refs):
    lo, hi = refs[-2:]
    acc = dot(a_ref[...], b_ref[...], TN)
    for i in range(adds):
        acc += refs[i][...]
    left = pl.program_id(0) < half

    @pl.when(left)
    def _():
        lo[...] = acc

    @pl.when(jnp.logical_not(left))
    def _():
        hi[...] = acc


def tn2_call(ids, a, b, adds, shape, place, into):
    t, dblk, ot = a.shape[0], 512, 1024
    n = b.shape[1] // ot
    half, off = n // 2, place // ot
    tile = pl.BlockSpec((dblk, ot), lambda j, s: (0, j))
    outs = [pl.BlockSpec((dblk, ot), lambda j, s: (0, jnp.minimum(j, half - 1) + off)),
            pl.BlockSpec((dblk, ot), lambda j, s: (0, jnp.maximum(j - half, 0) + off))]
    extra = list(into or ())
    return scalar_call(functools.partial(tn2_kernel, len(adds), half), (n,),
                       [pl.BlockSpec((t, dblk), lambda j, s: (0, s[0])), pl.BlockSpec((t, ot), lambda j, s: (0, j))]
                       + [tile] * len(adds) + [ANY] * len(extra), outs, [jax.ShapeDtypeStruct(shape, F32)] * 2,
                       alias={3 + len(adds) + k: k for k in range(len(extra))},
                       ce=cost(2 * t * dblk * b.shape[1], 2 * t * (dblk + b.shape[1]) + 12 * dblk * b.shape[1]))(
        ids, a, b, *adds, *extra)


def px(v):
    return lax.ppermute(v, 'fsdp', SWAP)


def py(v):
    return lax.ppermute(v, 'data', SWAP)


def pm(v):
    return lax.ppermute(v, 'model', SWAP)


def gather(axis, w):
    split = 1 - axis
    half = w.shape[split] // 2
    shape = list(w.shape)
    shape[axis] *= 4
    w_x = px(w)
    w_y = py(w)
    d_a = py(lax.slice_in_dim(w_x, 0, half, axis=split))
    d_b = px(lax.slice_in_dim(w_y, half, 2 * half, axis=split))
    return Weight(tuple(shape), axis, [(w, 0, 0), (w_x, 1, 0), (w_y, 2, 0), (d_a, 3, 0), (d_b, 3, half)])


def layer_impl(x_in, grad_out, gain_attn, gain_mlp, w_qkv, w_out, w_gate, w_up, w_down, rope_cos, rope_sin):
    batch, seq_loc, d_model = x_in.shape
    rows = batch * seq_loc
    width = w_qkv.shape[1]
    attn_w = w_out.shape[0]
    ffn = w_gate.shape[1]
    fh = ffn // 2
    me = lax.axis_index('data') * 2 + lax.axis_index('fsdp')
    core = lax.axis_index('model')
    ids = jnp.stack([me, me ^ 1, me ^ 2, me ^ 3, core, 1 - core]).astype(jnp.int32)
    own, oth = 4, 5

    x = x_in.reshape(rows, d_model)
    grad = grad_out.reshape(rows, d_model)
    g1, g2 = gain_attn.reshape(1, d_model), gain_mlp.reshape(1, d_model)
    one, zero = jnp.ones_like(rope_cos), jnp.zeros_like(rope_cos)
    cos_t = jnp.concatenate([rope_cos] * 10 + [one, one], axis=1).reshape(2, seq_loc, 6 * HEAD)
    sin_t = jnp.concatenate([-rope_sin, rope_sin] * 5 + [zero, zero], axis=1).reshape(2, seq_loc, 6 * HEAD)

    def both(v):
        return lax.all_gather(v, 'model', axis=0, tiled=True)

    def half_w(w, axis, i):
        return lax.slice_in_dim(w, i * fh, (i + 1) * fh, axis=axis)

    wq = gather(0, w_qkv)
    wo = gather(1, w_out)
    wgu, wd = [], []
    for i in range(2):
        wgu.append(gather(0, jnp.concatenate([half_w(w_gate, 1, i), half_w(w_up, 1, i)], axis=1)))
        wd.append(gather(1, half_w(w_down, 0, i)))

    h_s = rms_call(x, g1)
    h = both(h_s)
    g_full = both(grad)
    qkv = qkv_call(ids, h, wq, cos_t, sin_t).reshape(2, batch, seq_loc, width)
    o = attn_call(qkv).reshape(2 * rows, attn_w)
    part, = proj_call(ids, [o], [wo], NN, rows, oth, epi_round, [], 1)
    recv = pm(part)
    mid, h2_s = proj_call(ids, [o], [wo], NN, rows, own, epi_mid, [recv, x, g2], 2)
    h2 = both(h2_s)
    act, dgu = [None] * 2, [None] * 2
    for i in range(2):
        act[i], dgu[i] = mlp_call(ids, h2, g_full, wgu[i], wd[i])
    part, = proj_call(ids, act, wd, NN, rows, oth, epi_round, [], 1)
    recv = pm(part)
    y, = proj_call(ids, act, wd, NN, rows, own, epi_add, [recv, mid], 1)

    part, = proj_call(ids, dgu, wgu, NT, rows, oth, epi_round, [], 1)
    recv = pm(part)
    d_mid_s, = proj_call(ids, dgu, wgu, NT, rows, own, epi_rms_b, [recv, mid, grad, g2], 1)
    d_mid = both(d_mid_s)
    d_o, = proj_call(ids, [d_mid], [wo], NT, 2 * rows, None, epi_round, [], 1)
    d_qkv = attn_bwd_call(qkv, d_o.reshape(2, batch, seq_loc, attn_w), cos_t, sin_t).reshape(2 * rows, width)
    part, = proj_call(ids, [d_qkv], [wq], NT, rows, oth, epi_round, [], 1)
    recv = pm(part)
    dx, = proj_call(ids, [d_qkv], [wq], NT, rows, own, epi_rms_b, [recv, x, d_mid_s, g1], 1)

    def wsum(a, b, side, mode, last):
        first, second, j1, j2 = (px, py, 1, 2) if mode else (py, px, 2, 1)
        p3 = tn_call(ids, a, b, side, [3])
        r3 = first(p3)
        p1 = tn_call(ids, a, b, side, [j1])
        r1 = first(p1)
        p2 = tn_call(ids, a, b, side, [j2], [r3])
        r2 = second(p2)
        return last(r1, r2)

    dw_down = dw_gu = None
    for i in range(2):
        dw_down = wsum(act[i], g_full, 1, i == 0, lambda r1, r2: tn_call(
            ids, act[i], g_full, 1, [0], [r1, r2], dw_down, out_shape=(ffn, 512), place=i * fh))
        dw_gu = wsum(h2, dgu[i], 0, i == 1, lambda r1, r2: tn2_call(
            ids, h2, dgu[i], [r1, r2], (512, ffn), i * fh, dw_gu))
    dw_gate, dw_up = dw_gu
    dw_out = wsum(o, d_mid, 1, True, lambda r1, r2: tn_call(ids, o, d_mid, 1, [0]) + r1 + r2)
    dw_qkv = wsum(h, d_qkv, 0, False, lambda r1, r2: tn_call(ids, h, d_qkv, 0, [0]) + r1 + r2)
    return (y.reshape(x_in.shape), dx.reshape(x_in.shape), dw_qkv, dw_out, dw_gate, dw_up, dw_down)


def solution(mesh):
    act_spec = P(FSDP_AXES, 'model', None)
    col_spec = P(FSDP_AXES, 'model')
    row_spec = P('model', FSDP_AXES)
    vec_spec = P(None)
    table_spec = P(None, None)
    in_specs = (act_spec, act_spec, vec_spec, vec_spec, col_spec, row_spec, col_spec, col_spec, row_spec, table_spec, table_spec)
    out_specs = (act_spec, act_spec, col_spec, row_spec, col_spec, col_spec, row_spec)
    return jax.shard_map(layer_impl, mesh=mesh, in_specs=in_specs, out_specs=out_specs, check_vma=False)
```
